32 devices in a mesh: mc: 8 (over z, x), mr: 4 (over y, core).
Axes of the slice: x: 2, y: 2, z: 4, core: 2. Of those that a mesh axis runs over, the one named last changes fastest.
Arguments:
- column_panel: float32 [4096, 256], P('mc', 'mr'), may hold values from -0.375 to 0.375
- diag_block: float32 [256, 256], P('mc', 'mr'), may hold values from -4.3 to 4.3, as said below
- row_panel: float32 [256, 32768], P('mc', 'mr'), may hold values from -6 to 6
- trailing: float32 [4096, 32768], P('mc', 'mr'), may hold values from -6 to 6
Outputs:
- solved_panel: float32 [4096, 256], P('mc', 'mr')
- inverse_block: float32 [256, 256], P('mc', 'mr')
- scaled_panel: float32 [256, 32768], P('mc', 'mr')
- updated: float32 [4096, 32768], P('mc', 'mr')
The draws below stay inside these ranges and needn't reach their ends.
Inputs may be any that keep to these rules, and one draw needn't show every extreme that they name: `diag_block`: upper triangle with a diagonal of magnitude 2 to 4 and small off-diagonal entries.
All inputs are finite; a program needn't handle non-finite values.
Results may differ from the reference program's by a relative error of at most 0.00011.
Values sent between devices are 32-bit elements; how exact they have to be, the bound alone decides.
No kernel may reach another device: no remote copies, remote signals or barrier semaphores. Data moves between devices by JAX's collectives and lax.ppermute only.
A program may use at most 128 MiB of HBM per device.

```python
import jax
import jax.numpy as jnp
from jax import lax

B = 256
COLS = 32768
ROWS = 4096


def draw_diag_block(key, part):
    first, second, third = jax.random.split(key, 3)
    offdiag = 0.06 * jnp.clip(jax.random.normal(first, (B, B), jnp.float32), -5.0, 5.0)
    signs = jnp.where(jax.random.bernoulli(second, 0.5, (B,)), 1.0, -1.0).astype(jnp.float32)
    magnitude = jax.random.uniform(third, (B,), jnp.float32, 2.0, 4.0)
    keep = 1.0 - jnp.eye(B, dtype=jnp.float32)
    return offdiag * keep + jnp.diag(signs * magnitude)


def shard_levels(rng, extent, cuts, smallest, largest):
    loudness = 1.0
    for position, parts in cuts:
        steps = jax.random.uniform(jax.random.fold_in(jax.random.fold_in(rng, 6), position), (parts,), jnp.float32, smallest / len(cuts), largest / len(cuts))
        loudness = loudness * jnp.repeat(jnp.exp(steps), extent[position] // parts).reshape((-1,) + (1,) * (len(extent) - 1 - position))
    return loudness


def centred(rng, shape, deviation, reach, pieces=(), kind=jnp.bfloat16):
    array = deviation * jax.random.normal(rng, shape, jnp.float32)
    if pieces:
        array = array * shard_levels(rng, shape, pieces, -0.22, 0.18)
    return jnp.clip(array, -reach, reach).astype(kind)


def setup_inputs(seed: int = 0) -> dict:
    key_of = jax.random.split(jax.random.key(seed), 5)
    column_panel = centred(key_of[0], (ROWS, B), B ** -0.5, 0.375, ((0, 8), (1, 4)), jnp.float32)
    diag_block = draw_diag_block(jax.random.fold_in(key_of[4], 71), 0)
    row_panel = centred(key_of[2], (B, COLS), 1.0, 6.0, ((0, 8), (1, 4)), jnp.float32)
    trailing = centred(key_of[3], (ROWS, COLS), 1.0, 6.0, ((0, 8), (1, 4)), jnp.float32)
    return {"column_panel": column_panel, "diag_block": diag_block, "row_panel": row_panel, "trailing": trailing}


def reference(column_panel, diag_block, row_panel, trailing):
    upper = jnp.triu(diag_block)
    identity = jnp.eye(B, dtype=diag_block.dtype)
    inverse_block = jax.scipy.linalg.solve_triangular(upper, identity, lower=False)
    solved_panel = -jnp.dot(column_panel, inverse_block, precision=lax.Precision.HIGHEST)
    updated = trailing + jnp.dot(solved_panel, row_panel, precision=lax.Precision.HIGHEST)
    scaled_panel = jnp.dot(inverse_block, row_panel, precision=lax.Precision.HIGHEST)
    return (solved_panel, inverse_block, scaled_panel, updated)
```

```python
import functools

import jax
import jax.numpy as jnp
from jax import lax
from jax.experimental import pallas as pl
from jax.experimental.pallas import tpu as pltpu
from jax.sharding import PartitionSpec as P

F32 = jnp.float32
BF16 = jnp.bfloat16

CHUNKS = ((0.5, "x"), (1.5, "z"), (2, "x"), (2, "z"), (1.5, "x"), (0.5, "z"))


def exchange(array, mask, count):
    return lax.ppermute(array, "mc", [(i, i ^ mask) for i in range(count)])


def split(value):
    high = value.astype(BF16)
    low = (value - high.astype(F32)).astype(BF16)
    return high, low


def first_phase(block, kind, count):
    parts = {0: block}
    parts[1] = exchange(block, 1, count)
    parts[2] = exchange(block, 2, count)
    parts[4] = exchange(block, 4, count)
    if kind == "x":
        parts[6] = exchange(block, 6, count)
    return parts


def second_phase(parts, kind, count):
    rows = parts[0].shape[0]
    if kind == "x":
        sent = jnp.concatenate([parts[2], parts[4], parts[6]], 0)
        got = exchange(sent, 1, count)
        arrays = [parts[0], parts[1], parts[2], parts[4], parts[6], got]
        offsets = [(0,), (1,), (2,), (4,), (6,), (3, 5, 7)]
    else:
        mid = exchange(jnp.concatenate([parts[4], parts[1]], 0), 2, count)
        got = exchange(jnp.concatenate([parts[4], mid[:rows]], 0), 1, count)
        arrays = [parts[0], parts[1], parts[2], parts[4], mid, got]
        offsets = [(0,), (1,), (2,), (4,), (6, 3), (5, 7)]
    bit = 8
    while bit < count:
        held = jnp.concatenate(arrays, 0)
        flat = tuple(o for group in offsets for o in group)
        arrays = [held, exchange(held, bit, count)]
        offsets = [flat, tuple(o ^ bit for o in flat)]
        bit *= 2
    return arrays, offsets


def pack_kernel(offsets, width, rows, where_ref, column_ref, *refs):
    blocks, out_ref, hold = refs[: len(offsets)], refs[-2], refs[-1]
    me = where_ref[0]
    for block, group in zip(blocks, offsets):
        for i, offset in enumerate(group):
            row = pl.multiple_of((me ^ offset) * rows, rows)
            hold[pl.ds(row, rows), :] = block[i * rows : (i + 1) * rows, :]
    height = column_ref.shape[1]
    out_ref[:, :height] = column_ref[...]
    out_ref[:, height:] = hold[...].T[:width, :]


def prepare_kernel(block_rows, block_cols, where_ref, panel_ref, high_ref, low_ref, solved_ref, part_ref, hold, slim, wide):
    order = panel_ref.shape[0]
    height = panel_ref.shape[1] - order
    dot = functools.partial(jnp.dot, precision=lax.Precision.HIGHEST, preferred_element_type=F32)
    lower = panel_ref[:, height:]
    row = lax.broadcasted_iota(jnp.int32, (order, order), 0)
    col = lax.broadcasted_iota(jnp.int32, (order, order), 1)
    pivots = jnp.where(row == col, lower, 0.0)
    recip_row = 1.0 / jnp.sum(pivots, axis=0, keepdims=True)
    recip_col = 1.0 / jnp.sum(pivots, axis=1, keepdims=True)
    identity = jnp.where(row == col, 1.0, 0.0).astype(F32)
    power = -(jnp.where(row > col, lower, 0.0) * recip_row)
    product = identity + power
    for _ in range(max((order - 1).bit_length(), 1) - 1):
        power = dot(power, power)
        product = product + dot(product, power)
    inverse = recip_col * product
    wide[...] = -dot(inverse, panel_ref[:, :height])
    hold[...] = inverse
    me_row = pl.multiple_of(where_ref[0] * block_rows, block_rows)
    me_col = pl.multiple_of(where_ref[1] * block_cols, block_cols)
    solved_ref[...] = wide[pl.ds(me_col, block_cols), :]
    slim[...] = hold[pl.ds(me_col, block_cols), :].T
    part_ref[...] = slim[pl.ds(me_row, block_rows), :]
    hold[...] = inverse.T
    high, low = split(wide[...].T)
    high_ref[:height, :] = high
    low_ref[:height, :] = low
    high, low = split(hold[pl.ds(me_row, block_rows), :])
    high_ref[height:, :] = high
    low_ref[height:, :] = low


def update_kernel(offsets, rows, aliased, where_ref, high_ref, low_ref, trail_ref, *refs):
    blocks = refs[: len(offsets)]
    out_ref, scaled_ref, top, rest = refs[len(offsets) + (2 if aliased else 0) :]
    me = where_ref[0]
    for block, group in zip(blocks, offsets):
        for i, offset in enumerate(group):
            row = pl.multiple_of((me ^ offset) * rows, rows)
            high, low = split(block[i * rows : (i + 1) * rows, :])
            top[pl.ds(row, rows), :] = high
            rest[pl.ds(row, rows), :] = low
    dot = functools.partial(jnp.dot, preferred_element_type=F32)
    total = dot(high_ref[...], top[...])
    total = total + dot(high_ref[...], rest[...])
    total = total + dot(low_ref[...], top[...])
    height = out_ref.shape[0]
    out_ref[...] = trail_ref[...] + total[:height]
    scaled_ref[...] = total[height:]


def vmem(shape, index=None):
    if index is None:
        return pl.BlockSpec(shape, lambda *_: (0,) * len(shape))
    return pl.BlockSpec(shape, index)


def update_chunk(where, high, low, trailing, arrays, offsets, start, width, order, outs):
    rows = arrays[0].shape[0] // len(offsets[0])
    height, columns = trailing.shape
    tile = 512
    while width % tile or start % tile:
        tile //= 2
    first = start // tile
    at = lambda j, _: (0, first + j)
    here = lambda j, _: (0, j)
    specs = [vmem(high.shape), vmem(low.shape), vmem((height, tile), at)]
    specs += [vmem((a.shape[0], tile), here) for a in arrays]
    args = [high, low, trailing, *arrays]
    aliases = {}
    if outs is not None:
        specs += [pl.BlockSpec(memory_space=pl.ANY)] * 2
        aliases = {1 + len(args): 0, 2 + len(args): 1}
        args += list(outs)
    flops = 6 * high.shape[0] * order * width
    return pl.pallas_call(
        functools.partial(update_kernel, offsets, rows, outs is not None),
        out_shape=(
            jax.ShapeDtypeStruct((height, columns), F32),
            jax.ShapeDtypeStruct((rows, columns), F32),
        ),
        grid_spec=pltpu.PrefetchScalarGridSpec(
            num_scalar_prefetch=1,
            grid=(width // tile,),
            in_specs=specs,
            out_specs=(vmem((height, tile), at), vmem((rows, tile), at)),
            scratch_shapes=[pltpu.VMEM((order, tile), BF16)] * 2,
        ),
        input_output_aliases=aliases,
        cost_estimate=pl.CostEstimate(flops=flops, bytes_accessed=8 * height * width, transcendentals=0),
        name=f"update_{start}",
    )(where, *args)


def shards(sizes, column_panel, diag_block, row_panel, trailing):
    count = sizes["mc"]
    block_rows, block_cols = diag_block.shape
    order = block_rows * count
    height = column_panel.shape[0]
    columns = row_panel.shape[1]
    where = jnp.stack([lax.axis_index("mc"), lax.axis_index("mr")]).astype(jnp.int32)

    pad = -block_cols % 128
    unit = columns // 16
    starts, widths = [], []
    at = 0
    for eighths, _ in CHUNKS:
        starts.append(at)
        widths.append(int(eighths * 2) * unit)
        at += widths[-1]
    kinds = [kind for _, kind in CHUNKS]

    firsts, pieces = [], []
    for c, (start, width) in enumerate(zip(starts, widths)):
        block = row_panel[:, start : start + width]
        if c == 0:
            block = jnp.concatenate([block, diag_block, jnp.zeros((block_rows, pad), F32)], 1)
        if c >= 2:
            held = firsts[c - 2]
            keys = sorted(held)
            block, *values = lax.optimization_barrier((block, *[held[k] for k in keys]))
            firsts[c - 2] = dict(zip(keys, values))
        firsts.append(first_phase(block, kinds[c], count))

    for c in range(len(CHUNKS)):
        pieces.append(second_phase(firsts[c], kinds[c], count))

    arrays, offsets = pieces[0]
    lane = widths[0] // 128
    packed = pl.pallas_call(
        functools.partial(pack_kernel, offsets, block_cols, block_rows),
        out_shape=jax.ShapeDtypeStruct((block_cols, height + order), F32),
        grid_spec=pltpu.PrefetchScalarGridSpec(
            num_scalar_prefetch=1,
            grid=(1,),
            in_specs=[vmem((block_cols, height))]
            + [vmem((a.shape[0], block_cols + pad), lambda i, _: (0, widths[0] // (block_cols + pad))) for a in arrays],
            out_specs=vmem((block_cols, height + order)),
            scratch_shapes=[pltpu.VMEM((order, block_cols + pad), F32)],
        ),
        name="pack",
    )(where, column_panel.T, *arrays)
    panel = lax.all_gather(packed, "mr", axis=0, tiled=True)
    high, low, solved, part = pl.pallas_call(
        functools.partial(prepare_kernel, block_rows, block_cols),
        out_shape=(
            jax.ShapeDtypeStruct((height + block_rows, order), BF16),
            jax.ShapeDtypeStruct((height + block_rows, order), BF16),
            jax.ShapeDtypeStruct((block_cols, height), F32),
            jax.ShapeDtypeStruct((block_rows, block_cols), F32),
        ),
        grid_spec=pltpu.PrefetchScalarGridSpec(
            num_scalar_prefetch=1,
            grid=(1,),
            in_specs=[vmem(panel.shape)],
            out_specs=(
                vmem((height + block_rows, order)),
                vmem((height + block_rows, order)),
                vmem((block_cols, height)),
                vmem((block_rows, block_cols)),
            ),
            scratch_shapes=[
                pltpu.VMEM((order, order), F32),
                pltpu.VMEM((order, block_cols), F32),
                pltpu.VMEM((order, height), F32),
            ],
        ),
        cost_estimate=pl.CostEstimate(flops=2 * 14 * 6 * order**3, bytes_accessed=4 * panel.size, transcendentals=0),
        name="prepare",
    )(where, panel)

    outs = None
    for c in range(len(CHUNKS)):
        arrays, offsets = pieces[c]
        outs = update_chunk(where, high, low, trailing, arrays, offsets, starts[c], widths[c], order, outs)
    updated, scaled = outs
    return (solved.T, part, scaled, updated)


def solution(mesh):
    placed = P("mc", "mr")
    return jax.shard_map(
        functools.partial(shards, dict(mesh.shape)),
        mesh=mesh,
        in_specs=(placed,) * 4,
        out_specs=(placed,) * 4,
        check_vma=False,
    )
```
